512 devices in a mesh: row: 128 (over z, x, core), col: 4 (over y).
Axes of the slice: x: 4, y: 4, z: 16, core: 2. Of those that a mesh axis runs over, the one named last changes fastest.
Arguments:
- right_side: float32 [384, 131072], P(None, ('row', 'col')), may hold values from -51 to 51
- leaf_inverse: float32 [512, 256, 256], P(('row', 'col')), may hold values from -0.375 to 0.375
- leaf_diag: float32 [512, 256, 256], P(('row', 'col')), may hold values from -0.375 to 0.375
- node_block: float32 [512, 256, 256], P(('row', 'col')), may hold values from -0.375 to 0.375
Outputs:
- solution: float32 [384, 131072], P(None, ('row', 'col'))
- residual_norm: float32 [384], replicated
The draws below stay inside these ranges and needn't reach their ends.
All inputs are finite; a program needn't handle non-finite values.
Results may differ from the reference program's by a relative error of at most 0.0001.
Values sent between devices are 32-bit elements; how exact they have to be, the bound alone decides.
No kernel may reach another device: no remote copies, remote signals or barrier semaphores. Data moves between devices by JAX's collectives and lax.ppermute only.
A program may use at most 64 MiB of HBM per device.

```python
import jax
import jax.numpy as jnp
from jax import lax

LEAF = 256
NRHS = 384
NLEAF = 512
N = 131072
DEVICES = 512


def draw_right_side(key, part):
    key_values = jax.random.fold_in(jax.random.fold_in(key, 11), 0)
    rising = 1.0 + 2.0 * jnp.arange(N, dtype=jnp.float32) / (N - 1)
    values = jnp.clip(jax.random.normal(key_values, (NRHS, N), jnp.float32), -5.0, 5.0)
    return values * rising[None, :]


def steps_of(rng, shape, cuts, low, largest):
    level = 1.0
    for dim, parts in cuts:
        steps = jax.random.uniform(jax.random.fold_in(jax.random.fold_in(rng, 6), dim), (parts,), jnp.float32, low / len(cuts), largest / len(cuts))
        level = level * jnp.repeat(jnp.exp(steps), shape[dim] // parts).reshape((-1,) + (1,) * (len(shape) - 1 - dim))
    return level


def noise(own_key, extent, deviation, bound, cuts=(), kind=jnp.bfloat16):
    entries = jax.random.normal(own_key, extent, jnp.float32) * deviation
    if len(cuts) > 0:
        entries = steps_of(own_key, extent, cuts, -0.22, 0.18) * entries
    return jnp.clip(entries, min=-bound, max=bound).astype(kind)


def setup_inputs(seed: int = 0) -> dict:
    splits = jax.random.split(jax.random.key(seed), 5)
    return {
        "right_side": draw_right_side(jax.random.fold_in(splits[4], 71), 0),
        "leaf_inverse": noise(splits[1], (NLEAF, LEAF, LEAF), LEAF ** -0.5, 0.375, ((0, 512),), jnp.float32),
        "leaf_diag": noise(splits[2], (NLEAF, LEAF, LEAF), LEAF ** -0.5, 0.375, ((0, 512),), jnp.float32),
        "node_block": noise(splits[3], (DEVICES, LEAF, LEAF), LEAF ** -0.5, 0.375, ((0, 512),), jnp.float32),
    }


PRECISE = lax.Precision.HIGHEST

def forward(vectors, blocks):
    return jnp.einsum('ncl,nml->ncm', vectors, blocks, precision=PRECISE)

def backward(vectors, blocks):
    return jnp.einsum('ncm,nml->ncl', vectors, blocks, precision=PRECISE)

def reference(right_side, leaf_inverse, leaf_diag, node_block):
    leaf_count = leaf_inverse.shape[0]
    leaf_width = leaf_inverse.shape[1]
    half_width = leaf_width // 2
    rhs_count = right_side.shape[0]
    tree_depth = leaf_count.bit_length() - 1
    leaf_rhs = right_side.reshape(rhs_count, leaf_count, leaf_width).transpose(1, 0, 2)
    lifted = forward(leaf_rhs, leaf_inverse)
    leaf_part = lifted[..., :half_width]
    skeleton = lifted[..., half_width:]
    stored = []
    merged = lifted
    for tree_level in range(1, tree_depth + 1):
        node_count = leaf_count >> tree_level
        paired = skeleton.reshape(node_count, 2, rhs_count, half_width)
        joined = jnp.concatenate([paired[:, 0], paired[:, 1]], axis=-1)
        slot_index = jnp.arange(node_count, dtype=jnp.int32) * 2 ** tree_level + 2 ** (tree_level - 1)
        blocks = node_block[slot_index]
        merged = forward(joined, blocks)
        stored.append((merged[..., :half_width], blocks))
        skeleton = merged[..., half_width:]
    root_solved = forward(merged, node_block[0:1])
    known = jnp.stack([root_solved[0, :, :half_width], root_solved[0, :, half_width:]])
    for tree_level in range(tree_depth - 1, 0, -1):
        eliminated, blocks = stored[tree_level - 1]
        expanded = backward(jnp.concatenate([eliminated, known], axis=-1), blocks)
        node_count = expanded.shape[0]
        known = expanded.reshape(node_count, rhs_count, 2, half_width).transpose(0, 2, 1, 3)
        known = known.reshape(2 * node_count, rhs_count, half_width)
    solved = backward(jnp.concatenate([leaf_part, known], axis=-1), leaf_inverse)
    solution = solved.transpose(1, 0, 2).reshape(rhs_count, leaf_count * leaf_width)
    residual = leaf_rhs - forward(solved, leaf_diag)
    mean_square = lax.optimization_barrier(jnp.sum(residual * residual, axis=(0, 2))) / (leaf_count * leaf_width)
    return (solution, jnp.sqrt(mean_square + 1e-06))
```

```python
import jax
import jax.numpy as jnp
from jax import lax
from jax.sharding import Mesh
from jax.sharding import PartitionSpec as P


ALL = ("z", "x", "c", "y")
PLANE = ("x", "c", "y")
PRECISE = lax.Precision.HIGHEST


def swapped(block, axis, bit):
    count = lax.axis_size(axis)
    return lax.ppermute(block, axis, [(i, i ^ bit) for i in range(count)])


def direct(parts, axes):
    return lax.all_to_all(parts, axes, 0, 0)


def to_each(value, axes):
    count = lax.axis_size(axes)
    return direct(jnp.broadcast_to(value[None], (count,) + value.shape), axes)


def powers(count):
    return [1 << k for k in range(count.bit_length() - 1)]


def apply_block(vectors, block):
    return lax.dot_general(
        vectors,
        block,
        (((1,), (1,)), ((), ())),
        precision=PRECISE,
        preferred_element_type=jnp.float32,
    )


def apply_transpose(vectors, block):
    return jnp.dot(vectors, block, precision=PRECISE, preferred_element_type=jnp.float32)


def pick(is_left, values, half):
    return jnp.where(is_left, values[:, :half], values[:, half:])


def joined(is_left, own, other):
    return jnp.concatenate(
        [jnp.where(is_left, own, other), jnp.where(is_left, other, own)], axis=1
    )


def body(right_side, leaf_inverse, leaf_diag, node_block):
    z = lax.axis_index("z")
    planes = lax.axis_size("z")
    depth = planes.bit_length() - 1
    members = lax.axis_size(PLANE)
    member = lax.axis_index(PLANE)
    leaf_block = leaf_inverse[0]
    own_block = node_block[0]
    rhs, width = right_side.shape
    half = width // 2

    groups = lax.axis_size("x")
    group = members // groups

    rows = width // members
    scattered = direct(own_block.reshape(members, rows, width), PLANE)
    along = to_each(scattered[0], "z")
    homes = [0] + [(z >> k << k) + (1 << (k - 1)) for k in range(1, depth + 1)]
    slices = [scattered[i * group] for i in range(1, groups)]
    slices += [lax.dynamic_index_in_dim(along, h, 0, False) for h in homes]
    gathered = to_each(jnp.stack(slices), PLANE)
    whole = [gathered[:, k].reshape(width, width) for k in range(len(slices))]
    across, top = [None] + whole[: groups - 1], whole[groups - 1 :]

    chain = own_block
    skeleton = apply_block(right_side, leaf_block[half:])
    leaf_part = apply_block(right_side, leaf_block[:half])
    lower = []
    for axis in ("y", "c"):
        for bit in powers(lax.axis_size(axis)):
            is_left = (lax.axis_index(axis) & bit) == 0
            other_block = swapped(chain, axis, bit)
            block = jnp.where(is_left, other_block, chain)
            chain = jnp.where(is_left, chain, other_block)
            other = swapped(skeleton, axis, bit)
            mine, theirs = pick(is_left, block, half), pick(~is_left, block, half)
            eliminated = apply_block(skeleton, mine[:half]) + apply_block(other, theirs[:half])
            skeleton = apply_block(skeleton, mine[half:]) + apply_block(other, theirs[half:])
            lower.append((is_left, block, eliminated))

    x = lax.axis_index("x")
    share = rhs // members
    shares = skeleton.reshape(groups, group, share, half)
    shares = lax.dynamic_index_in_dim(shares, member % group, 1, False)
    own = [lax.dynamic_index_in_dim(shares, x, 0, False)]
    for m in range(1, groups):
        part = lax.dynamic_index_in_dim(shares, x ^ m, 0, False)
        own.append(swapped(part, "x", m))
    for bit in powers(groups):
        swap = (x & bit) != 0
        own = [jnp.where(swap, own[i ^ bit], own[i]) for i in range(groups)]
    middle = []
    for bit in powers(groups):
        blocks = [across[(2 * i + 1) * bit] for i in range(groups // (2 * bit))]
        merged = [
            apply_block(jnp.concatenate(own[2 * i : 2 * i + 2], axis=1), block)
            for i, block in enumerate(blocks)
        ]
        middle.append((blocks, [m[:, :half] for m in merged]))
        own = [m[:, half:] for m in merged]
    own = own[0]

    sides = [(z >> k & 1) == 0 for k in range(depth)]
    lifts = [own]
    for k in range(1, depth):
        lifts.append(apply_block(lifts[-1], pick(sides[k - 1], top[k][half:], half)))
    distance = z ^ jnp.arange(planes, dtype=jnp.int32)
    sent = jnp.broadcast_to(lifts[0][None], (planes, share, half))
    for k in range(1, depth):
        sent = jnp.where((distance >> k != 0)[:, None, None], lifts[k][None], sent)
    got = direct(sent, "z")
    stored = []
    for k in range(1, depth + 1):
        from_sibling = (distance >> (k - 1)) == 1
        other = jnp.sum(jnp.where(from_sibling[:, None, None], got, 0.0), axis=0)
        merged = apply_block(joined(sides[k - 1], own, other), top[k])
        stored.append(merged[:, :half])
        own = merged[:, half:]
    known = pick(sides[depth - 1], apply_block(merged, top[0]), half)
    for k in range(depth - 1, 0, -1):
        expanded = apply_transpose(jnp.concatenate([stored[k - 1], known], axis=1), top[k])
        known = pick(sides[k - 1], expanded, half)

    known = [known]
    for blocks, parts in reversed(middle):
        expanded = [
            apply_transpose(jnp.concatenate([part, value], axis=1), block)
            for block, part, value in zip(blocks, parts, known)
        ]
        known = [v for e in expanded for v in (e[:, :half], e[:, half:])]
    known = jnp.stack(known)[:, None]
    known = jnp.broadcast_to(known, (groups, group, share, half))
    known = direct(known.reshape(members, share, half), PLANE).reshape(rhs, half)
    for is_left, block, eliminated in reversed(lower):
        expanded = apply_transpose(jnp.concatenate([eliminated, known], axis=1), block)
        known = pick(is_left, expanded, half)
    solved = apply_transpose(jnp.concatenate([leaf_part, known], axis=1), leaf_block)
    residual = right_side - apply_block(solved, leaf_diag[0])
    squares = jnp.sum(residual * residual, axis=1).reshape(-1, 128)
    totals = jnp.sum(to_each(squares, PLANE), axis=0)
    totals = jnp.sum(to_each(totals, "z"), axis=0).reshape(-1)
    residual_norm = jnp.sqrt(totals / (planes * members * width) + 1e-06)
    return (solved, residual_norm)


def solution(mesh):
    finer = Mesh(mesh.devices.reshape(16, 4, 2, mesh.shape["col"]), ALL)
    placed = (P(None, ALL), P(ALL, None, None), P(ALL, None, None), P(ALL, None, None))
    return jax.shard_map(
        body, mesh=finer, in_specs=placed, out_specs=(P(None, ALL), P()), check_vma=False
    )
```

```python
import functools

import jax
import jax.numpy as jnp
from jax import lax
from jax.experimental import pallas as pl
from jax.experimental.pallas import tpu as pltpu
from jax.sharding import Mesh
from jax.sharding import PartitionSpec as P


ALL = ("z", "x", "c", "y")
PLANE = ("x", "c", "y")
PRECISE = lax.Precision.HIGHEST


def swapped(block, axis, bit):
    count = lax.axis_size(axis)
    return lax.ppermute(block, axis, [(i, i ^ bit) for i in range(count)])


def direct(parts, axes):
    return lax.all_to_all(parts, axes, 0, 0)


def to_each(value, axes):
    count = lax.axis_size(axes)
    return direct(jnp.broadcast_to(value[None], (count,) + value.shape), axes)


def powers(count):
    return [1 << k for k in range(count.bit_length() - 1)]


def apply_block(vectors, block):
    return lax.dot_general(
        vectors,
        block,
        (((1,), (1,)), ((), ())),
        precision=PRECISE,
        preferred_element_type=jnp.float32,
    )


def apply_transpose(vectors, block):
    return jnp.dot(vectors, block, precision=PRECISE, preferred_element_type=jnp.float32)


def pick(is_left, values, half):
    return jnp.where(is_left, values[:, :half], values[:, half:])


LIMIT = 16 * 2**20
COST = pl.CostEstimate(flops=40_000_000, bytes_accessed=3_000_000, transcendentals=0)


def whole(gathered_ref, k):
    block = gathered_ref[:, k]
    return block.reshape(block.shape[0] * block.shape[1], block.shape[2])


def halves(value, half):
    return value[:, :half], value[:, half:]


def beside(first, second):
    return jnp.concatenate([first, second], axis=1)


def rise(groups, planes, *refs):
    own_refs, (gathered_ref, sent_ref, own_ref, middle_ref) = refs[:groups], refs[groups:]
    half = sent_ref.shape[-1]
    x, z = lax.axis_index("x"), lax.axis_index("z")
    own = [ref[...] for ref in own_refs]
    for bit in powers(groups):
        swap = (x & bit) != 0
        own = [jnp.where(swap, own[i ^ bit], own[i]) for i in range(groups)]
    for bit in powers(groups):
        above = []
        for i in range(groups // (2 * bit)):
            node = (2 * i + 1) * bit
            merged = apply_block(beside(own[2 * i], own[2 * i + 1]), whole(gathered_ref, node - 1))
            middle_ref[node - 1], skeleton = halves(merged, half)
            above.append(skeleton)
        own = above
    own_ref[...] = own[0]
    lifts = [own[0]]
    for k in range(1, planes.bit_length() - 1):
        low = whole(gathered_ref, groups - 1 + k)[half:]
        lifts.append(apply_block(lifts[-1], pick((z >> (k - 1) & 1) == 0, low, half)))
    for i in range(planes):
        value = lifts[0]
        for k in range(1, len(lifts)):
            value = jnp.where((z ^ i) >> k != 0, lifts[k], value)
        sent_ref[i] = value


def fall(groups, planes, got_ref, own_ref, middle_ref, gathered_ref, known_ref):
    half = own_ref.shape[-1]
    depth = planes.bit_length() - 1
    z = lax.axis_index("z")
    sides = [(z >> k & 1) == 0 for k in range(depth)]
    own = own_ref[...]
    stored = []
    for k in range(1, depth + 1):
        span = 1 << (k - 1)
        first = ((z >> (k - 1)) ^ 1) << (k - 1)
        other = got_ref[first]
        for i in range(1, span):
            other = other + got_ref[first + i]
        left, right = jnp.where(sides[k - 1], own, other), jnp.where(sides[k - 1], other, own)
        merged = apply_block(beside(left, right), whole(gathered_ref, groups - 1 + k))
        eliminated, own = halves(merged, half)
        stored.append(eliminated)
    count = gathered_ref.shape[0] // 2
    root = gathered_ref[pl.ds((z >> (depth - 1)) * count, count), groups - 1]
    known = apply_block(merged, root.reshape(half, 2 * half))
    for k in range(depth - 1, 0, -1):
        mine = pick(sides[k - 1], whole(gathered_ref, groups - 1 + k), half)
        known = apply_transpose(beside(stored[k - 1], known), mine)
    known = [known]
    for bit in reversed(powers(groups)):
        below = []
        for i, value in enumerate(known):
            node = (2 * i + 1) * bit
            expanded = apply_transpose(
                beside(middle_ref[node - 1], value), whole(gathered_ref, node - 1)
            )
            below += halves(expanded, half)
        known = below
    group = known_ref.shape[0] // groups
    for i, value in enumerate(known):
        for j in range(group):
            known_ref[i * group + j] = value


def body(right_side, leaf_inverse, leaf_diag, node_block):
    z = lax.axis_index("z")
    planes = lax.axis_size("z")
    depth = planes.bit_length() - 1
    members = lax.axis_size(PLANE)
    member = lax.axis_index(PLANE)
    leaf_block = leaf_inverse[0]
    own_block = node_block[0]
    rhs, width = right_side.shape
    half = width // 2

    groups = lax.axis_size("x")
    group = members // groups

    rows = width // members
    scattered = direct(own_block.reshape(members, rows, width), PLANE)
    along = to_each(scattered[0], "z")
    homes = [0] + [(z >> k << k) + (1 << (k - 1)) for k in range(1, depth + 1)]
    slices = [scattered[i * group] for i in range(1, groups)]
    slices += [lax.dynamic_index_in_dim(along, h, 0, False) for h in homes]
    gathered = to_each(jnp.stack(slices), PLANE)

    x = lax.axis_index("x")
    share = rhs // members
    stretch = groups * share
    first = (member % group) * stretch
    chain = halves(own_block, half)
    skeleton = apply_block(right_side, leaf_block[half:])
    leaf_part = apply_block(right_side, leaf_block[:half])
    lower = []
    hops = [(axis, bit) for axis in ("y", "c") for bit in powers(lax.axis_size(axis))]
    for axis, bit in hops:
        is_left = (lax.axis_index(axis) & bit) == 0
        if (axis, bit) == hops[0]:
            other_chain = halves(swapped(own_block, axis, bit), half)
            other = swapped(skeleton, axis, bit)
        else:
            packed = swapped(jnp.concatenate((skeleton,) + chain), axis, bit)
            other = packed[:rhs]
            other_chain = packed[rhs : rhs + width], packed[rhs + width :]
        block = [jnp.where(is_left, o, m) for o, m in zip(other_chain, chain)]
        chain = tuple(jnp.where(is_left, m, o) for o, m in zip(other_chain, chain))
        mine, theirs = jnp.where(is_left, *block), jnp.where(is_left, *reversed(block))
        eliminated = apply_block(skeleton, mine[:half]) + apply_block(other, theirs[:half])
        if (axis, bit) == hops[-1]:
            skeleton = lax.dynamic_slice_in_dim(skeleton, first, stretch, 0)
            other = lax.dynamic_slice_in_dim(other, first, stretch, 0)
        skeleton = apply_block(skeleton, mine[half:]) + apply_block(other, theirs[half:])
        lower.append((mine, eliminated))

    shares = skeleton.reshape(groups, share, half)
    own = [lax.dynamic_index_in_dim(shares, x, 0, False)]
    for m in range(1, groups):
        part = lax.dynamic_index_in_dim(shares, x ^ m, 0, False)
        own.append(swapped(part, "x", m))
    kernel = functools.partial(rise, groups, planes)
    small = jax.ShapeDtypeStruct((groups, share, half), jnp.float32)
    sent, own, middle = pl.pallas_call(
        kernel,
        out_shape=(
            jax.ShapeDtypeStruct((planes, share, half), jnp.float32),
            jax.ShapeDtypeStruct((share, half), jnp.float32),
            small,
        ),
        in_specs=[pl.BlockSpec(memory_space=pltpu.VMEM)] * (groups + 1),
        out_specs=(pl.BlockSpec(memory_space=pltpu.VMEM),) * 3,
        cost_estimate=COST,
        compiler_params=pltpu.CompilerParams(vmem_limit_bytes=LIMIT),
    )(*own, gathered)
    got = direct(sent, "z")
    kernel = functools.partial(fall, groups, planes)
    known = pl.pallas_call(
        kernel,
        out_shape=jax.ShapeDtypeStruct((members, share, half), jnp.float32),
        in_specs=[pl.BlockSpec(memory_space=pltpu.VMEM)] * 4,
        out_specs=pl.BlockSpec(memory_space=pltpu.VMEM),
        cost_estimate=COST,
        compiler_params=pltpu.CompilerParams(vmem_limit_bytes=LIMIT),
    )(got, own, middle, gathered)
    known = direct(known, PLANE).reshape(groups, group, share, half)
    known = jnp.swapaxes(known, 0, 1).reshape(rhs, half)
    for mine, eliminated in reversed(lower):
        known = apply_transpose(eliminated, mine[:half]) + apply_transpose(known, mine[half:])
    solved = apply_transpose(jnp.concatenate([leaf_part, known], axis=1), leaf_block)
    residual = right_side - apply_block(solved, leaf_diag[0])
    squares = jnp.sum(residual * residual, axis=1).reshape(-1, 128)
    totals = jnp.sum(to_each(squares, PLANE), axis=0)
    totals = jnp.sum(to_each(totals, "z"), axis=0).reshape(-1)
    residual_norm = jnp.sqrt(totals / (planes * members * width) + 1e-06)
    return (solved, residual_norm)


def solution(mesh):
    finer = Mesh(mesh.devices.reshape(16, 4, 2, mesh.shape["col"]), ALL)
    placed = (P(None, ALL), P(ALL, None, None), P(ALL, None, None), P(ALL, None, None))
    return jax.shard_map(
        body, mesh=finer, in_specs=placed, out_specs=(P(None, ALL), P()), check_vma=False
    )
```

```python
import functools

import jax
import jax.numpy as jnp
from jax import lax
from jax.experimental import pallas as pl
from jax.experimental.pallas import tpu as pltpu
from jax.sharding import Mesh
from jax.sharding import PartitionSpec as P


ALL = ("z", "x", "c", "y")
PLANE = ("x", "c", "y")
PRECISE = lax.Precision.HIGHEST


def swapped(block, axis, bit):
    count = lax.axis_size(axis)
    return lax.ppermute(block, axis, [(i, i ^ bit) for i in range(count)])


def direct(parts, axes):
    return lax.all_to_all(parts, axes, 0, 0)


def to_each(value, axes):
    count = lax.axis_size(axes)
    return direct(jnp.broadcast_to(value[None], (count,) + value.shape), axes)


def powers(count):
    return [1 << k for k in range(count.bit_length() - 1)]


def apply_block(vectors, block):
    return lax.dot_general(
        vectors,
        block,
        (((1,), (1,)), ((), ())),
        precision=PRECISE,
        preferred_element_type=jnp.float32,
    )


def apply_transpose(vectors, block):
    return jnp.dot(vectors, block, precision=PRECISE, preferred_element_type=jnp.float32)


def pick(is_left, values, half):
    return jnp.where(is_left, values[:, :half], values[:, half:])


LIMIT = 16 * 2**20
COST = pl.CostEstimate(flops=40_000_000, bytes_accessed=3_000_000, transcendentals=0)


def rows_of(ref, k):
    block = ref[:, k]
    return block.reshape(block.shape[0] * block.shape[1], block.shape[2])


def halves(value, half):
    return value[:, :half], value[:, half:]


def beside(first, second):
    return jnp.concatenate([first, second], axis=1)


def by_core(compute, mine_ref, theirs_ref):
    core = lax.axis_index("c")
    for owner, refs in ((0, (mine_ref, theirs_ref)), (1, (theirs_ref, mine_ref))):
        pl.when(core == owner)(functools.partial(compute, *refs))


def rise(groups, planes, *refs):
    own_refs = refs[:groups]
    mine_ref, theirs_ref, sent_ref, own_ref, middle_ref = refs[groups:]
    half = sent_ref.shape[-1]
    x, z = lax.axis_index("x"), lax.axis_index("z")

    def compute(upper_ref, lower_ref):
        own = [ref[...] for ref in own_refs]
        for bit in powers(groups):
            swap = (x & bit) != 0
            own = [jnp.where(swap, own[i ^ bit], own[i]) for i in range(groups)]
        for bit in powers(groups):
            above = []
            for i in range(groups // (2 * bit)):
                node = (2 * i + 1) * bit - 1
                joint = beside(own[2 * i], own[2 * i + 1])
                middle_ref[node] = apply_block(joint, rows_of(upper_ref, node))
                above.append(apply_block(joint, rows_of(lower_ref, node)))
            own = above
        own_ref[...] = own[0]
        lifts = [own[0]]
        for k in range(1, planes.bit_length() - 1):
            low = pick((z >> (k - 1) & 1) == 0, rows_of(lower_ref, groups - 1 + k), half)
            lifts.append(apply_block(lifts[-1], low))
        for i in range(planes):
            value = lifts[0]
            for k in range(1, len(lifts)):
                value = jnp.where((z ^ i) >> k != 0, lifts[k], value)
            sent_ref[i] = value

    by_core(compute, mine_ref, theirs_ref)


def fall(groups, planes, got_ref, own_ref, middle_ref, mine_ref, theirs_ref, known_ref):
    half = own_ref.shape[-1]
    depth = planes.bit_length() - 1
    group = known_ref.shape[0] // groups
    z = lax.axis_index("z")
    sides = [(z >> k & 1) == 0 for k in range(depth)]

    def compute(upper_ref, lower_ref):
        own = own_ref[...]
        stored = []
        for k in range(1, depth + 1):
            start = ((z >> (k - 1)) ^ 1) << (k - 1)
            other = got_ref[start]
            for i in range(1, 1 << (k - 1)):
                other = other + got_ref[start + i]
            joint = beside(
                jnp.where(sides[k - 1], own, other), jnp.where(sides[k - 1], other, own)
            )
            stored.append(apply_block(joint, rows_of(upper_ref, groups - 1 + k)))
            own = apply_block(joint, rows_of(lower_ref, groups - 1 + k))
        upper, lower = rows_of(upper_ref, groups - 1), rows_of(lower_ref, groups - 1)
        root = jnp.where(sides[depth - 1], upper, lower)
        known = apply_block(beside(stored[-1], own), root)
        for k in range(depth - 1, 0, -1):
            upper = pick(sides[k - 1], rows_of(upper_ref, groups - 1 + k), half)
            lower = pick(sides[k - 1], rows_of(lower_ref, groups - 1 + k), half)
            known = apply_transpose(stored[k - 1], upper) + apply_transpose(known, lower)
        known = [known]
        for bit in reversed(powers(groups)):
            below = []
            for i, value in enumerate(known):
                node = (2 * i + 1) * bit - 1
                expanded = apply_transpose(middle_ref[node], rows_of(upper_ref, node))
                expanded = expanded + apply_transpose(value, rows_of(lower_ref, node))
                below += halves(expanded, half)
            known = below
        for i, value in enumerate(known):
            for j in range(group):
                known_ref[j * groups + i] = value

    by_core(compute, mine_ref, theirs_ref)


def body(right_side, leaf_inverse, leaf_diag, node_block):
    z = lax.axis_index("z")
    planes = lax.axis_size("z")
    depth = planes.bit_length() - 1
    members = lax.axis_size(PLANE)
    member = lax.axis_index(PLANE)
    leaf_block = leaf_inverse[0]
    own_block = node_block[0]
    rhs, width = right_side.shape
    half = width // 2

    groups = lax.axis_size("x")
    group = members // groups

    rows = width // members
    scattered = direct(own_block.reshape(members, rows, width), ("c", "x", "y"))
    along = to_each(scattered[0], "z")
    homes = [0] + [(z >> k << k) + (1 << (k - 1)) for k in range(1, depth + 1)]
    slices = [scattered[i * lax.axis_size("y")] for i in range(1, groups)]
    slices += [lax.dynamic_index_in_dim(along, h, 0, False) for h in homes]
    blocks = to_each(jnp.stack(slices), ("x", "y"))
    blocks = (blocks, swapped(blocks, "c", 1))

    x = lax.axis_index("x")
    share = rhs // members
    stretch = groups * share
    first = (member % group) * stretch
    chain = own_block
    skeleton = apply_block(right_side, leaf_block[half:])
    leaf_part = apply_block(right_side, leaf_block[:half])
    lower = []
    hops = [(axis, bit) for axis in ("y", "c") for bit in powers(lax.axis_size(axis))]
    for axis, bit in hops:
        is_left = (lax.axis_index(axis) & bit) == 0
        other_chain = swapped(chain, axis, bit)
        other = swapped(skeleton, axis, bit)
        mine = jnp.where(is_left, other_chain[:, :half], chain[:, half:])
        theirs = jnp.where(is_left, other_chain[:, half:], chain[:, :half])
        chain = jnp.where(is_left, chain, other_chain)
        eliminated = apply_block(skeleton, mine[:half]) + apply_block(other, theirs[:half])
        if (axis, bit) == hops[-1]:
            skeleton = lax.dynamic_slice_in_dim(skeleton, first, stretch, 0)
            other = lax.dynamic_slice_in_dim(other, first, stretch, 0)
        skeleton = apply_block(skeleton, mine[half:]) + apply_block(other, theirs[half:])
        lower.append((mine, eliminated))

    shares = skeleton.reshape(groups, share, half)
    own = [lax.dynamic_index_in_dim(shares, x, 0, False)]
    for m in range(1, groups):
        part = lax.dynamic_index_in_dim(shares, x ^ m, 0, False)
        own.append(swapped(part, "x", m))
    kernel = functools.partial(rise, groups, planes)
    small = jax.ShapeDtypeStruct((groups, share, half), jnp.float32)
    sent, own, middle = pl.pallas_call(
        kernel,
        out_shape=(
            jax.ShapeDtypeStruct((planes, share, half), jnp.float32),
            jax.ShapeDtypeStruct((share, half), jnp.float32),
            small,
        ),
        in_specs=[pl.BlockSpec(memory_space=pltpu.VMEM)] * (groups + 2),
        out_specs=(pl.BlockSpec(memory_space=pltpu.VMEM),) * 3,
        cost_estimate=COST,
        compiler_params=pltpu.CompilerParams(vmem_limit_bytes=LIMIT),
    )(*own, *blocks)
    got = direct(sent, "z")
    kernel = functools.partial(fall, groups, planes)
    known = pl.pallas_call(
        kernel,
        out_shape=jax.ShapeDtypeStruct((members, share, half), jnp.float32),
        in_specs=[pl.BlockSpec(memory_space=pltpu.VMEM)] * 5,
        out_specs=pl.BlockSpec(memory_space=pltpu.VMEM),
        cost_estimate=COST,
        compiler_params=pltpu.CompilerParams(vmem_limit_bytes=LIMIT),
    )(got, own, middle, *blocks)
    known = direct(known, ("c", "y", "x")).reshape(rhs, half)
    for mine, eliminated in reversed(lower):
        known = apply_transpose(eliminated, mine[:half]) + apply_transpose(known, mine[half:])
    solved = apply_transpose(jnp.concatenate([leaf_part, known], axis=1), leaf_block)
    residual = right_side - apply_block(solved, leaf_diag[0])
    squares = jnp.sum(residual * residual, axis=1).reshape(-1, 128)
    totals = jnp.sum(to_each(squares, PLANE), axis=0)
    totals = jnp.sum(to_each(totals, "z"), axis=0).reshape(-1)
    residual_norm = jnp.sqrt(totals / (planes * members * width) + 1e-06)
    return (solved, residual_norm)


def solution(mesh):
    finer = Mesh(mesh.devices.reshape(16, 4, 2, mesh.shape["col"]), ALL)
    placed = (P(None, ALL), P(ALL, None, None), P(ALL, None, None), P(ALL, None, None))
    return jax.shard_map(
        body, mesh=finer, in_specs=placed, out_specs=(P(None, ALL), P()), check_vma=False
    )
```

```python
import functools

import jax
import jax.numpy as jnp
from jax import lax
from jax.experimental import pallas as pl
from jax.experimental.pallas import tpu as pltpu
from jax.sharding import Mesh
from jax.sharding import PartitionSpec as P


ALL = ("z", "x", "c", "y")
PLANE = ("x", "c", "y")
PRECISE = lax.Precision.HIGHEST


def swapped(block, axis, bit):
    count = lax.axis_size(axis)
    return lax.ppermute(block, axis, [(i, i ^ bit) for i in range(count)])


def direct(parts, axes):
    return lax.all_to_all(parts, axes, 0, 0)


def to_each(value, axes):
    count = lax.axis_size(axes)
    return direct(jnp.broadcast_to(value[None], (count,) + value.shape), axes)


def powers(count):
    return [1 << k for k in range(count.bit_length() - 1)]


def apply_block(vectors, block):
    return lax.dot_general(
        vectors,
        block,
        (((1,), (1,)), ((), ())),
        precision=PRECISE,
        preferred_element_type=jnp.float32,
    )


def apply_transpose(vectors, block):
    return jnp.dot(vectors, block, precision=PRECISE, preferred_element_type=jnp.float32)


def pick(is_left, values, half):
    return jnp.where(is_left, values[:, :half], values[:, half:])


LIMIT = 16 * 2**20
COST = pl.CostEstimate(flops=40_000_000, bytes_accessed=3_000_000, transcendentals=0)


def rows_of(ref, k):
    block = ref[:, k]
    return block.reshape(block.shape[0] * block.shape[1], block.shape[2])


def halves(value, half):
    return value[:, :half], value[:, half:]


def beside(first, second):
    return jnp.concatenate([first, second], axis=1)


def by_core(compute, mine_ref, theirs_ref):
    core = lax.axis_index("c")
    for owner, refs in ((0, (mine_ref, theirs_ref)), (1, (theirs_ref, mine_ref))):
        pl.when(core == owner)(functools.partial(compute, *refs))


def rise(groups, planes, *refs):
    own_refs = refs[:groups]
    mine_ref, theirs_ref, sent_ref, own_ref, middle_ref = refs[groups:]
    half = sent_ref.shape[-1]
    x, z = lax.axis_index("x"), lax.axis_index("z")

    def compute(upper_ref, lower_ref):
        own = [ref[...] for ref in own_refs]
        for bit in powers(groups):
            swap = (x & bit) != 0
            own = [jnp.where(swap, own[i ^ bit], own[i]) for i in range(groups)]
        for bit in powers(groups):
            above = []
            for i in range(groups // (2 * bit)):
                node = (2 * i + 1) * bit - 1
                joint = beside(own[2 * i], own[2 * i + 1])
                middle_ref[node] = apply_block(joint, rows_of(upper_ref, node))
                above.append(apply_block(joint, rows_of(lower_ref, node)))
            own = above
        own_ref[...] = own[0]
        lifts = [own[0]]
        for k in range(1, planes.bit_length() - 1):
            low = pick((z >> (k - 1) & 1) == 0, rows_of(lower_ref, groups - 1 + k), half)
            lifts.append(apply_block(lifts[-1], low))
        for i in range(planes):
            value = lifts[0]
            for k in range(1, len(lifts)):
                value = jnp.where((z ^ i) >> k != 0, lifts[k], value)
            sent_ref[i] = value

    by_core(compute, mine_ref, theirs_ref)


def fall(groups, planes, got_ref, own_ref, middle_ref, mine_ref, theirs_ref, known_ref):
    half = own_ref.shape[-1]
    depth = planes.bit_length() - 1
    group = known_ref.shape[0] // groups
    z = lax.axis_index("z")
    sides = [(z >> k & 1) == 0 for k in range(depth)]

    def compute(upper_ref, lower_ref):
        own = own_ref[...]
        stored = []
        for k in range(1, depth + 1):
            start = ((z >> (k - 1)) ^ 1) << (k - 1)
            other = got_ref[start]
            for i in range(1, 1 << (k - 1)):
                other = other + got_ref[start + i]
            joint = beside(
                jnp.where(sides[k - 1], own, other), jnp.where(sides[k - 1], other, own)
            )
            stored.append(apply_block(joint, rows_of(upper_ref, groups - 1 + k)))
            own = apply_block(joint, rows_of(lower_ref, groups - 1 + k))
        upper, lower = rows_of(upper_ref, groups - 1), rows_of(lower_ref, groups - 1)
        root = jnp.where(sides[depth - 1], upper, lower)
        known = apply_block(beside(stored[-1], own), root)
        for k in range(depth - 1, 0, -1):
            upper = pick(sides[k - 1], rows_of(upper_ref, groups - 1 + k), half)
            lower = pick(sides[k - 1], rows_of(lower_ref, groups - 1 + k), half)
            known = apply_transpose(stored[k - 1], upper) + apply_transpose(known, lower)
        known = [known]
        for bit in reversed(powers(groups)):
            below = []
            for i, value in enumerate(known):
                node = (2 * i + 1) * bit - 1
                expanded = apply_transpose(middle_ref[node], rows_of(upper_ref, node))
                expanded = expanded + apply_transpose(value, rows_of(lower_ref, node))
                below += halves(expanded, half)
            known = below
        for i, value in enumerate(known):
            for j in range(group):
                known_ref[j * groups + i] = value

    by_core(compute, mine_ref, theirs_ref)


def body(right_side, leaf_inverse, leaf_diag, node_block):
    z = lax.axis_index("z")
    planes = lax.axis_size("z")
    depth = planes.bit_length() - 1
    members = lax.axis_size(PLANE)
    member = lax.axis_index(PLANE)
    leaf_block = leaf_inverse[0]
    own_block = node_block[0]
    rhs, width = right_side.shape
    half = width // 2

    groups = lax.axis_size("x")
    group = members // groups

    rows = width // members
    scattered = direct(own_block.reshape(members, rows, width), ("c", "x", "y"))
    along = to_each(scattered[0], "z")
    homes = [0] + [(z >> k << k) + (1 << (k - 1)) for k in range(1, depth + 1)]
    slices = [scattered[i * lax.axis_size("y")] for i in range(1, groups)]
    slices += [lax.dynamic_index_in_dim(along, h, 0, False) for h in homes]
    blocks = to_each(jnp.stack(slices), ("x", "y"))
    blocks = (blocks, swapped(blocks, "c", 1))

    x = lax.axis_index("x")
    share = rhs // members
    stretch = groups * share
    first = (member % group) * stretch
    chain = own_block
    skeleton = apply_block(right_side, leaf_block[half:])
    leaf_part = apply_block(right_side, leaf_block[:half])
    lower = []
    hops = [(axis, bit) for axis in ("y", "c") for bit in powers(lax.axis_size(axis))]
    for axis, bit in hops:
        is_left = (lax.axis_index(axis) & bit) == 0
        other_chain = swapped(chain, axis, bit)
        other = swapped(skeleton, axis, bit)
        mine = jnp.where(is_left, other_chain[:, :half], chain[:, half:])
        theirs = jnp.where(is_left, other_chain[:, half:], chain[:, :half])
        chain = jnp.where(is_left, chain, other_chain)
        eliminated = apply_block(skeleton, mine[:half]) + apply_block(other, theirs[:half])
        part = apply_transpose(eliminated, mine[:half])
        if (axis, bit) == hops[-1]:
            skeleton = lax.dynamic_slice_in_dim(skeleton, first, stretch, 0)
            other = lax.dynamic_slice_in_dim(other, first, stretch, 0)
        skeleton = apply_block(skeleton, mine[half:]) + apply_block(other, theirs[half:])
        lower.append((mine[half:], part))

    through = lower[-1][0]
    for block, _ in reversed(lower[:-1]):
        through = apply_transpose(through, block)
    through = apply_transpose(through, leaf_block[half:])
    rest = lower[-1][1]
    for block, part in reversed(lower[:-1]):
        rest = part + apply_transpose(rest, block)
    rest = apply_transpose(rest, leaf_block[half:])
    rest = rest + apply_transpose(leaf_part, leaf_block[:half])

    shares = skeleton.reshape(groups, share, half)
    own = [lax.dynamic_index_in_dim(shares, x, 0, False)]
    for m in range(1, groups):
        part = lax.dynamic_index_in_dim(shares, x ^ m, 0, False)
        own.append(swapped(part, "x", m))
    kernel = functools.partial(rise, groups, planes)
    small = jax.ShapeDtypeStruct((groups, share, half), jnp.float32)
    sent, own, middle = pl.pallas_call(
        kernel,
        out_shape=(
            jax.ShapeDtypeStruct((planes, share, half), jnp.float32),
            jax.ShapeDtypeStruct((share, half), jnp.float32),
            small,
        ),
        in_specs=[pl.BlockSpec(memory_space=pltpu.VMEM)] * (groups + 2),
        out_specs=(pl.BlockSpec(memory_space=pltpu.VMEM),) * 3,
        cost_estimate=COST,
        compiler_params=pltpu.CompilerParams(vmem_limit_bytes=LIMIT),
    )(*own, *blocks)
    got = direct(sent, "z")
    kernel = functools.partial(fall, groups, planes)
    known = pl.pallas_call(
        kernel,
        out_shape=jax.ShapeDtypeStruct((members, share, half), jnp.float32),
        in_specs=[pl.BlockSpec(memory_space=pltpu.VMEM)] * 5,
        out_specs=pl.BlockSpec(memory_space=pltpu.VMEM),
        cost_estimate=COST,
        compiler_params=pltpu.CompilerParams(vmem_limit_bytes=LIMIT),
    )(got, own, middle, *blocks)
    known = direct(known, ("c", "y", "x")).reshape(rhs, half)
    solved = rest + apply_transpose(known, through)
    residual = right_side - apply_block(solved, leaf_diag[0])
    squares = jnp.sum(residual * residual, axis=1).reshape(-1, 128)
    totals = jnp.sum(to_each(squares, PLANE), axis=0)
    totals = jnp.sum(to_each(totals, "z"), axis=0).reshape(-1)
    residual_norm = jnp.sqrt(totals / (planes * members * width) + 1e-06)
    return (solved, residual_norm)


def solution(mesh):
    finer = Mesh(mesh.devices.reshape(16, 4, 2, mesh.shape["col"]), ALL)
    placed = (P(None, ALL), P(ALL, None, None), P(ALL, None, None), P(ALL, None, None))
    return jax.shard_map(
        body, mesh=finer, in_specs=placed, out_specs=(P(None, ALL), P()), check_vma=False
    )
```
